32 devices in a mesh: dp: 4 (over x, core), tensor: 8 (over z, y).
Axes of the slice: x: 2, y: 2, z: 4, core: 2. Of those that a mesh axis runs over, the one named last changes fastest.
Arguments:
- attn_out: bfloat16 [96, 8192], P('dp', 'tensor'), parts along dimension 0, may hold values from -6 to 6
- w_out: bfloat16 [8192, 7168], P('tensor'), may hold values from -0.0625 to 0.0625
- residual: bfloat16 [96, 7168], P(('dp', 'tensor')), parts along dimension 0, may hold values from -6 to 6
- norm_gain: float32 [7168], replicated, may hold values from 0.1 to 1.9
Outputs:
- new_stream: bfloat16 [96, 7168], P(('dp', 'tensor')), parts along dimension 0
- quantized: bfloat16 [96, 7168], P(('dp', 'tensor')), parts along dimension 0
- block_scales: float32 [96, 56], P(('dp', 'tensor')), parts along dimension 0
The draws below stay inside these ranges and needn't reach their ends.
There are 4 independent parts, one for each index of `dp`. The reference program is written for one: setup_inputs(seed, part) draws one part's arguments, and reference() takes and returns one part's arrays. A program takes and returns all parts, laid end to end along the dimension named above; an argument that names none is the same for every part. Nothing has to cross between parts.
All inputs are finite; a program needn't handle non-finite values. Where the reference program divides by a largest or mean magnitude, that divisor is 1e-20 or more.
Results may differ from the reference program's by a relative error of at most 0.0014.
Values sent between devices are 32-bit elements; how exact they have to be, the bound alone decides.
No kernel may reach another device: no remote copies, remote signals or barrier semaphores. Data moves between devices by JAX's collectives and lax.ppermute only.
A program may use at most 64 MiB of HBM per device.

```python
import jax
import jax.numpy as jnp
from jax import lax

D = 7168
HEADS = 64
HD = 128
BLOCK = 128
TOKENS = 24


def raised(result, own_key, source, target, blocks, factor):
    def block_of(dim):
        return (jnp.arange(result.shape[dim]) // (result.shape[dim] // blocks)).reshape((-1,) + (1,) * (result.ndim - 1 - dim))

    near = jax.random.permutation(own_key, blocks)[block_of(target)]
    other_side = (block_of(target) + blocks // 2) % blocks
    return jnp.where((block_of(source) == near) | (block_of(source) == other_side), factor * result, result)


def block_scale(rng, dims, shards, low, top_value):
    level, own = 1.0, jax.random.fold_in(rng, 6)
    for position, shards_of in shards:
        steps = jnp.exp(jax.random.uniform(jax.random.fold_in(own, position), (shards_of,), jnp.float32, low / len(shards), top_value / len(shards)))
        level = level * jnp.repeat(steps, dims[position] // shards_of).reshape([-1 if axis == position else 1 for axis in range(len(dims))])
    return level


def gaussian(rng, shape, scale, reach, cuts=(), dtype=jnp.bfloat16):
    gain = block_scale(rng, shape, cuts, -0.22, 0.18) if cuts else 1.0
    entries = jax.random.normal(rng, shape, jnp.float32) * scale * gain
    return jnp.minimum(jnp.maximum(entries, -reach), reach).astype(dtype)


def noise_with(stream_key, dims, scale, bound, pieces, heavy, dtype=jnp.bfloat16):
    array = scale * jax.random.normal(stream_key, dims, jnp.float32)
    if pieces:
        array = array * block_scale(stream_key, dims, pieces, -0.22, 0.18)
    return jnp.clip(raised(array, jax.random.fold_in(stream_key, 3), *heavy), -bound, bound).astype(dtype)


def setup_inputs(seed: int = 0, part: int = 0) -> dict:
    key_list = jax.random.split(jax.random.key(seed), 5)
    part_keys = jax.random.split(jax.random.fold_in(key_list[4], part), 5)
    attn_out = noise_with(part_keys[0], (TOKENS, HEADS * HD), 1.0, 6.0, ((1, 8),), (1, 0, 8, 2.0))
    w_out = gaussian(key_list[1], (HEADS * HD, D), (HEADS * HD) ** -0.5, 0.0625, ((0, 8),))
    residual = gaussian(part_keys[2], (TOKENS, D), 1.0, 6.0, ((0, 8),))
    norm_gain = jnp.clip(1.0 + 0.18 * jax.random.normal(key_list[3], (D,), jnp.float32), 0.1, 1.9)
    return dict(attn_out=attn_out, w_out=w_out, residual=residual, norm_gain=norm_gain)


def finish(hidden, norm_gain):
    count = hidden.shape[0]
    width = hidden.shape[1]
    new_stream = hidden.astype(jnp.bfloat16)
    mean_square = lax.optimization_barrier(jnp.mean(hidden * hidden, axis=1, keepdims=True))
    normed = hidden * lax.rsqrt(mean_square + 1e-06) * norm_gain
    blocks = normed.reshape(count, width // BLOCK, BLOCK)
    peak_abs = lax.optimization_barrier(jnp.max(jnp.abs(blocks), axis=2)) + 1e-06
    quantized = (blocks * 448.0 / peak_abs[:, :, None]).reshape(count, width).astype(jnp.bfloat16)
    return (new_stream, quantized, peak_abs / 448.0)

def reference(attn_out, w_out, residual, norm_gain):
    projected = jnp.dot(attn_out, w_out, preferred_element_type=jnp.float32)
    hidden = residual.astype(jnp.float32) + projected
    return finish(hidden, norm_gain)
```

```python
import functools
import jax
import jax.numpy as jnp
from jax import lax
from jax.experimental import pallas as pl
from jax.experimental.pallas import tpu as pltpu
from jax.sharding import PartitionSpec as P

BLOCK = 128
AXIS = "tensor"


def product_kernel(order, rows, strip, attn_ref, w_ref, out_ref, w_buf, sems):
    tokens = attn_ref.shape[0]
    width = w_ref.shape[1]
    blocks = width // BLOCK
    strips = width // strip
    copies = [
        pltpu.make_async_copy(
            w_ref.at[:, pl.ds(s * strip, strip)], w_buf.at[s], sems.at[s]
        )
        for s in range(strips)
    ]
    for copy in copies:
        copy.start()
    me = lax.axis_index(AXIS)
    pos = lax.broadcasted_iota(jnp.int32, (tokens, tokens), 0)
    col = lax.broadcasted_iota(jnp.int32, (tokens, tokens), 1)
    slot = pos // rows
    member = jnp.zeros_like(slot)
    for place, mask in enumerate(order):
        member = jnp.where(slot == place, mask, member)
    want = (member ^ me) * rows + (pos - slot * rows)
    pick = jnp.where(col == want, 1.0, 0.0).astype(jnp.bfloat16)
    mine = jnp.dot(pick, attn_ref[...], preferred_element_type=jnp.float32).astype(jnp.bfloat16)
    for s in range(strips):
        copies[s].wait()
        acc = jnp.dot(mine, w_buf[s], preferred_element_type=jnp.float32)
        for c in range(strip // BLOCK):
            out_ref[pl.ds(s * (strip // BLOCK) + c, tokens, stride=blocks), :] = acc[:, c * BLOCK : (c + 1) * BLOCK]


def product(attn, w, order, rows):
    tokens, depth = attn.shape
    width = w.shape[1]
    strip = 512 if width % 512 == 0 else BLOCK
    strips = width // strip
    return pl.pallas_call(
        functools.partial(product_kernel, order, rows, strip),
        out_shape=jax.ShapeDtypeStruct((tokens * width // BLOCK, BLOCK), jnp.float32),
        in_specs=[pl.BlockSpec(memory_space=pltpu.VMEM), pl.BlockSpec(memory_space=pl.ANY)],
        out_specs=pl.BlockSpec(memory_space=pltpu.VMEM),
        scratch_shapes=[
            pltpu.VMEM((strips, depth, strip), jnp.bfloat16),
            pltpu.SemaphoreType.DMA((strips,)),
        ],
        compiler_params=pltpu.CompilerParams(vmem_limit_bytes=40 * 1024 * 1024),
        cost_estimate=pl.CostEstimate(flops=2 * tokens * depth * width, bytes_accessed=2 * depth * width, transcendentals=0),
        name="product",
    )(attn, w)


def tail_kernel(rows, base_ref, got_ref, gain_ref, new_ref, quant_ref, scale_ref, hid, nrm):
    blocks = gain_ref.shape[0]
    for j in range(rows):
        at = pl.ds(j * blocks, blocks)
        hidden = base_ref[at, :] + got_ref[at, :]
        hid[at, :] = hidden
        total = jnp.sum(hidden * hidden, axis=(0, 1), keepdims=True)
        normed = hidden * lax.rsqrt(total / (blocks * BLOCK) + 1e-06) * gain_ref[...]
        peak = jnp.max(jnp.abs(normed), axis=1, keepdims=True) + 1e-06
        nrm[at, :] = normed * 448.0 / peak
        scale_ref[pl.ds(j, 1), :] = jnp.transpose(jnp.broadcast_to(peak / 448.0, (blocks, BLOCK)))[:1, :]
    for c in range(blocks):
        lanes = pl.ds(c * BLOCK, BLOCK)
        new_ref[:, lanes] = hid[pl.ds(c, rows, stride=blocks), :].astype(jnp.bfloat16)
        quant_ref[:, lanes] = nrm[pl.ds(c, rows, stride=blocks), :].astype(jnp.bfloat16)


def tail(base, got, gain, rows):
    blocks = gain.shape[0]
    width = blocks * BLOCK
    return pl.pallas_call(
        functools.partial(tail_kernel, rows),
        out_shape=(
            jax.ShapeDtypeStruct((rows, width), jnp.bfloat16),
            jax.ShapeDtypeStruct((rows, width), jnp.bfloat16),
            jax.ShapeDtypeStruct((rows, blocks), jnp.float32),
        ),
        in_specs=[pl.BlockSpec(memory_space=pltpu.VMEM)] * 3,
        out_specs=[pl.BlockSpec(memory_space=pltpu.VMEM)] * 3,
        scratch_shapes=[pltpu.VMEM((rows * blocks, BLOCK), jnp.float32)] * 2,
        name="tail",
    )(base, got, gain)


def local(attn_out, w_out, residual, norm_gain):
    groups = lax.axis_size(AXIS)
    rows, width = residual.shape
    blocks = width // BLOCK
    near = min(4, groups)
    far = groups // near
    order = [f * near + q for q in range(near) for f in range(far)]

    def swap(value, mask):
        return lax.ppermute(value, AXIS, [(i, i ^ mask) for i in range(groups)])

    buf = product(attn_out, w_out, order, rows)
    quarter = buf.shape[0] // near
    parts = [buf[q * quarter : (q + 1) * quarter] for q in range(near)]
    got = [swap(parts[q], q) for q in range(1, near)]
    mine = parts[0]
    for g in got:
        mine = mine + g
    base = residual.astype(jnp.float32).reshape(rows * blocks, BLOCK)
    mask = groups // 2
    last = jnp.zeros_like(base)
    while mask >= near:
        half = mine.shape[0] // 2
        last = swap(mine[half:], mask)
        mine = mine[:half]
        if mask > near:
            mine = mine + last
        mask //= 2
    return tail(base + mine, last, norm_gain.reshape(blocks, BLOCK), rows)


def solution(mesh):
    return jax.shard_map(
        local,
        mesh=mesh,
        in_specs=(P("dp", "tensor"), P("tensor", None), P(("dp", "tensor"), None), P()),
        out_specs=(P(("dp", "tensor"), None), P(("dp", "tensor"), None), P(("dp", "tensor"), None)),
        check_vma=False,
    )
```

```python
import functools
import jax
import jax.numpy as jnp
from jax import lax
from jax.experimental import pallas as pl
from jax.experimental.pallas import tpu as pltpu
from jax.sharding import PartitionSpec as P

BLOCK = 128
AXIS = "tensor"
MIB = 1024 * 1024


def up(value, step):
    return -(-value // step) * step


def product_kernel(order, rows, first, strip, attn_hbm, w_ref, *refs):
    near = len(order)
    outs, (attn_ref, w_buf, sems, attn_sem) = refs[:near], refs[near:]
    tokens = attn_ref.shape[0]
    held = tokens // near
    lot = up(held, 8)
    blocks = outs[0].shape[0] // held
    strips = blocks // strip
    fetch = pltpu.make_async_copy(attn_hbm, attn_ref, attn_sem)
    fetch.start()
    copies = [
        pltpu.make_async_copy(
            w_ref.at[:, pl.ds((first + s * strip) * BLOCK, strip * BLOCK)], w_buf.at[s], sems.at[s]
        )
        for s in range(strips)
    ]
    for copy in copies:
        copy.start()
    me = lax.axis_index(AXIS)
    pos = lax.broadcasted_iota(jnp.int32, (lot * near, tokens), 0)
    col = lax.broadcasted_iota(jnp.int32, (lot * near, tokens), 1)
    want = jnp.full_like(pos, -1)
    for q, masks in enumerate(order):
        for f, mask in enumerate(masks):
            start = q * lot + f * rows
            here = (pos >= start) & (pos < start + rows)
            want = jnp.where(here, (me ^ mask) * rows + pos - start, want)
    pick = jnp.where(col == want, 1.0, 0.0).astype(jnp.bfloat16)
    fetch.wait()
    mine = jnp.dot(pick, attn_ref[...], preferred_element_type=jnp.float32).astype(jnp.bfloat16)
    for s in range(strips):
        copies[s].wait()
        acc = jnp.dot(mine, w_buf[s], preferred_element_type=jnp.float32)
        for c in range(strip):
            for q in range(near):
                outs[q][pl.ds(s * strip + c, held, stride=blocks), :] = acc[
                    q * lot : q * lot + held, c * BLOCK : (c + 1) * BLOCK
                ]


def product(attn, w, order, rows, first, blocks):
    tokens, depth = attn.shape
    near = len(order)
    strip = next(s for s in (4, 2, 1) if blocks % s == 0)
    part = jax.ShapeDtypeStruct((tokens // near * blocks, BLOCK), jnp.float32)
    return pl.pallas_call(
        functools.partial(product_kernel, order, rows, first, strip),
        out_shape=[part] * near,
        in_specs=[pl.BlockSpec(memory_space=pl.ANY)] * 2,
        out_specs=[pl.BlockSpec(memory_space=pltpu.VMEM)] * near,
        scratch_shapes=[
            pltpu.VMEM((tokens, depth), jnp.bfloat16),
            pltpu.VMEM((blocks // strip, depth, strip * BLOCK), jnp.bfloat16),
            pltpu.SemaphoreType.DMA((blocks // strip,)),
            pltpu.SemaphoreType.DMA,
        ],
        compiler_params=pltpu.CompilerParams(vmem_limit_bytes=40 * MIB),
        cost_estimate=pl.CostEstimate(
            flops=2 * tokens * depth * blocks * BLOCK, bytes_accessed=2 * depth * blocks * BLOCK, transcendentals=0
        ),
        name="product",
    )(attn, w)


def fold_kernel(near, widths, rows, *refs):
    ins, (keep_ref, send_ref) = refs[:-2], refs[-2:]
    total = sum(widths)
    at = 0
    for k, blocks in enumerate(widths):
        group = ins[k * near : (k + 1) * near]
        slots = group[0].shape[0] // blocks
        for t in range(slots):
            lines = pl.ds(t * blocks, blocks)
            value = group[0][lines, :]
            for ref in group[1:]:
                value = value + ref[lines, :]
            out, spot = (keep_ref, t) if t < slots // 2 else (send_ref, t - slots // 2)
            out[pl.ds(spot * total + at, blocks), :] = value
        at += blocks


def fold(groups, widths, rows):
    near = len(groups[0])
    lines = sum(g[0].shape[0] for g in groups) // 2
    part = jax.ShapeDtypeStruct((lines, BLOCK), jnp.float32)
    return pl.pallas_call(
        functools.partial(fold_kernel, near, widths, rows),
        out_shape=[part] * 2,
        in_specs=[pl.BlockSpec(memory_space=pltpu.VMEM)] * (near * len(groups)),
        out_specs=[pl.BlockSpec(memory_space=pltpu.VMEM)] * 2,
        compiler_params=pltpu.CompilerParams(vmem_limit_bytes=12 * MIB),
        name="fold",
    )(*[value for group in groups for value in group])


def tail_kernel(rows, keep_ref, res_ref, gain_ref, got_ref, new_ref, quant_ref, scale_ref, hid, nrm):
    blocks = gain_ref.shape[0]
    line = lax.broadcasted_iota(jnp.int32, (blocks, BLOCK), 0)
    lane = lax.broadcasted_iota(jnp.int32, (blocks, BLOCK), 1)
    for j in range(rows):
        at = pl.ds(j * blocks, blocks)
        hidden = keep_ref[at, :] + got_ref[at, :] + res_ref[at, :]
        hid[at, :] = hidden
        square = jnp.sum(jnp.sum(hidden * hidden, axis=0, keepdims=True), axis=1, keepdims=True)
        normed = hidden * lax.rsqrt(square / (blocks * BLOCK) + 1e-06) * gain_ref[...]
        peak = jnp.max(jnp.abs(normed), axis=1, keepdims=True) + 1e-06
        nrm[at, :] = normed * 448.0 / peak
        spread = jnp.where(line == lane, peak / 448.0, 0.0)
        scale_ref[pl.ds(j, 1), :] = jnp.sum(spread, axis=0, keepdims=True)[:, :blocks]
    for c in range(blocks):
        lanes = pl.ds(c * BLOCK, BLOCK)
        new_ref[:, lanes] = hid[pl.ds(c, rows, stride=blocks), :].astype(jnp.bfloat16)
        quant_ref[:, lanes] = nrm[pl.ds(c, rows, stride=blocks), :].astype(jnp.bfloat16)


def tail(keep, res, gain, got, rows):
    blocks = gain.shape[0]
    width = blocks * BLOCK
    return pl.pallas_call(
        functools.partial(tail_kernel, rows),
        out_shape=(
            jax.ShapeDtypeStruct((rows, width), jnp.bfloat16),
            jax.ShapeDtypeStruct((rows, width), jnp.bfloat16),
            jax.ShapeDtypeStruct((rows, blocks), jnp.float32),
        ),
        in_specs=[pl.BlockSpec(memory_space=pltpu.VMEM)] * 4,
        out_specs=[pl.BlockSpec(memory_space=pltpu.VMEM)] * 3,
        scratch_shapes=[pltpu.VMEM((rows * blocks, BLOCK), jnp.float32)] * 2,
        compiler_params=pltpu.CompilerParams(vmem_limit_bytes=8 * MIB),
        name="tail",
    )(keep, res, gain, got)


def local(attn_out, w_out, residual, norm_gain):
    groups = lax.axis_size(AXIS)
    rows, width = residual.shape
    blocks = width // BLOCK
    near = min(4, groups // 2)
    order = [[f * near + q for f in range(groups // near)] for q in range(near)]

    def swap(value, mask):
        return lax.ppermute(value, AXIS, [(i, i ^ mask) for i in range(groups)])

    widths = [blocks]
    collected = []
    first = 0
    for wide in widths:
        parts = product(attn_out, w_out, order, rows, first, wide)
        collected.append([parts[0]] + [swap(parts[q], q) for q in range(1, near)])
        first += wide
    keep, send = fold(collected, widths, rows)

    mask = groups // 2
    while mask > near:
        half = keep.shape[0] // 2
        moved = swap(send, mask)
        keep, send = keep[:half] + moved[:half], keep[half:] + moved[half:]
        mask //= 2
    res = residual.astype(jnp.float32).reshape(rows * blocks, BLOCK)
    return tail(keep, res, norm_gain.reshape(blocks, BLOCK), swap(send, mask), rows)


def solution(mesh):
    return jax.shard_map(
        local,
        mesh=mesh,
        in_specs=(P("dp", "tensor"), P("tensor", None), P(("dp", "tensor"), None), P()),
        out_specs=(P(("dp", "tensor"), None), P(("dp", "tensor"), None), P(("dp", "tensor"), None)),
        check_vma=False,
    )
```

```python
import functools
import jax
import jax.numpy as jnp
from jax import lax
from jax.experimental import pallas as pl
from jax.experimental.pallas import tpu as pltpu
from jax.sharding import PartitionSpec as P

BLOCK = 128
AXIS = "tensor"
PARTS = "dp"
MIB = 1024 * 1024
LEAD = 2
TURNS = ((0, 1, 2, 3), (0, 3, 2, 1))
STRIP = 4


def turned(near, q, odd):
    return TURNS[odd][q] if near == 4 else q


def up(value, step):
    return -(-value // step) * step


def product_kernel(near, far, rows, strips, attn_hbm, w_ref, *refs):
    outs, (attn_ref, w_buf, sems, attn_sem) = refs[:near], refs[near:]
    tokens = attn_ref.shape[0]
    held = tokens // near
    lot = up(held, 8)
    blocks = outs[0].shape[0] // held
    fetch = pltpu.make_async_copy(attn_hbm, attn_ref, attn_sem)
    fetch.start()
    spans = [pl.ds(start * BLOCK, wide * BLOCK) for start, wide in strips]
    copies = [pltpu.make_async_copy(w_ref.at[:, span], w_buf.at[:, span], sems.at[s]) for s, span in enumerate(spans)]
    for copy in copies[:LEAD]:
        copy.start()
    me = lax.axis_index(AXIS)
    pos = lax.broadcasted_iota(jnp.int32, (lot * near, tokens), 0)
    col = lax.broadcasted_iota(jnp.int32, (lot * near, tokens), 1)
    want = jnp.full_like(pos, -1)
    odd = lax.rem(lax.axis_index(PARTS), 2)
    for q in range(near):
        mask = jnp.where(odd == 1, turned(near, q, 1), turned(near, q, 0))
        for f in range(far):
            start = q * lot + f * rows
            here = (pos >= start) & (pos < start + rows)
            want = jnp.where(here, (me ^ (mask + f * near)) * rows + pos - start, want)
    pick = jnp.where(col == want, 1.0, 0.0).astype(jnp.bfloat16)
    fetch.wait()
    for copy in copies[LEAD:]:
        copy.start()
    mine = jnp.dot(pick, attn_ref[...], preferred_element_type=jnp.float32).astype(jnp.bfloat16)
    for s, (start, wide) in enumerate(strips):
        copies[s].wait()
        acc = jnp.dot(mine, w_buf[:, spans[s]], preferred_element_type=jnp.float32)
        for c in range(wide):
            for q in range(near):
                outs[q][pl.ds(start + c, held, stride=blocks), :] = acc[
                    q * lot : q * lot + held, c * BLOCK : (c + 1) * BLOCK
                ]


def cut(blocks):
    return [(start, min(STRIP, blocks - start)) for start in range(0, blocks, STRIP)]


def product(attn, w, near, rows):
    tokens, depth = attn.shape
    width = w.shape[1]
    far = tokens // (near * rows)
    strips = cut(width // BLOCK)
    part = jax.ShapeDtypeStruct((tokens // near * width // BLOCK, BLOCK), jnp.float32)
    return pl.pallas_call(
        functools.partial(product_kernel, near, far, rows, strips),
        out_shape=[part] * near,
        in_specs=[pl.BlockSpec(memory_space=pl.ANY)] * 2,
        out_specs=[pl.BlockSpec(memory_space=pltpu.VMEM)] * near,
        scratch_shapes=[
            pltpu.VMEM((tokens, depth), jnp.bfloat16),
            pltpu.VMEM((depth, width), jnp.bfloat16),
            pltpu.SemaphoreType.DMA((len(strips),)),
            pltpu.SemaphoreType.DMA,
        ],
        compiler_params=pltpu.CompilerParams(vmem_limit_bytes=40 * MIB),
        cost_estimate=pl.CostEstimate(
            flops=2 * tokens * depth * width, bytes_accessed=2 * depth * width, transcendentals=0
        ),
        name="product",
    )(pltpu.with_memory_space_constraint(attn, pltpu.HBM), pltpu.with_memory_space_constraint(w, pltpu.HBM))


def fold_kernel(*refs):
    ins, (keep_ref, send_ref) = refs[:-2], refs[-2:]
    half = keep_ref.shape[0]
    for out, start in ((keep_ref, 0), (send_ref, half)):
        lines = pl.ds(start, half)
        value = ins[0][lines, :]
        for ref in ins[1:]:
            value = value + ref[lines, :]
        out[...] = value


def fold(parts):
    half = jax.ShapeDtypeStruct((parts[0].shape[0] // 2, BLOCK), jnp.float32)
    return pl.pallas_call(
        fold_kernel,
        out_shape=[half] * 2,
        in_specs=[pl.BlockSpec(memory_space=pltpu.VMEM)] * len(parts),
        out_specs=[pl.BlockSpec(memory_space=pltpu.VMEM)] * 2,
        compiler_params=pltpu.CompilerParams(vmem_limit_bytes=12 * MIB),
        name="fold",
    )(*parts)


def tail_kernel(rows, keep_ref, res_ref, gain_ref, got_ref, new_ref, quant_ref, scale_ref, hid, nrm):
    blocks = gain_ref.shape[0]
    line = lax.broadcasted_iota(jnp.int32, (blocks, BLOCK), 0)
    lane = lax.broadcasted_iota(jnp.int32, (blocks, BLOCK), 1)
    for j in range(rows):
        at = pl.ds(j * blocks, blocks)
        hidden = keep_ref[at, :] + got_ref[at, :] + res_ref[at, :]
        hid[at, :] = hidden
        square = jnp.sum(jnp.sum(hidden * hidden, axis=0, keepdims=True), axis=1, keepdims=True)
        normed = hidden * lax.rsqrt(square / (blocks * BLOCK) + 1e-06) * gain_ref[...]
        peak = jnp.max(jnp.abs(normed), axis=1, keepdims=True) + 1e-06
        nrm[at, :] = normed * 448.0 / peak
        spread = jnp.where(line == lane, peak / 448.0, 0.0)
        scale_ref[pl.ds(j, 1), :] = jnp.sum(spread, axis=0, keepdims=True)[:, :blocks]
    for c in range(blocks):
        lanes = pl.ds(c * BLOCK, BLOCK)
        new_ref[:, lanes] = hid[pl.ds(c, rows, stride=blocks), :].astype(jnp.bfloat16)
        quant_ref[:, lanes] = nrm[pl.ds(c, rows, stride=blocks), :].astype(jnp.bfloat16)


def tail(keep, res, gain, got, rows):
    blocks = gain.shape[0]
    width = blocks * BLOCK
    return pl.pallas_call(
        functools.partial(tail_kernel, rows),
        out_shape=(
            jax.ShapeDtypeStruct((rows, width), jnp.bfloat16),
            jax.ShapeDtypeStruct((rows, width), jnp.bfloat16),
            jax.ShapeDtypeStruct((rows, blocks), jnp.float32),
        ),
        in_specs=[pl.BlockSpec(memory_space=pltpu.VMEM)] * 4,
        out_specs=[pl.BlockSpec(memory_space=pltpu.VMEM)] * 3,
        scratch_shapes=[pltpu.VMEM((rows * blocks, BLOCK), jnp.float32)] * 2,
        compiler_params=pltpu.CompilerParams(vmem_limit_bytes=8 * MIB),
        name="tail",
    )(keep, res, gain, got)


def local(attn_out, w_out, residual, norm_gain):
    groups = lax.axis_size(AXIS)
    rows, width = residual.shape
    blocks = width // BLOCK
    near = min(4, groups // 2)
    parts_of = lax.axis_size(PARTS)

    def swap(value, q):
        mask = lambda d: turned(near, q, d % 2) if q < near else q
        pairs = [(d * groups + i, d * groups + (i ^ mask(d))) for d in range(parts_of) for i in range(groups)]
        return lax.ppermute(value, (PARTS, AXIS), pairs)

    parts = product(attn_out, w_out, near, rows)
    keep, send = fold([parts[0]] + [swap(parts[q], q) for q in range(1, near)])
    mask = groups // 2
    while mask > near:
        half = keep.shape[0] // 2
        moved = swap(send, mask)
        keep, send = keep[:half] + moved[:half], keep[half:] + moved[half:]
        mask //= 2
    res = residual.astype(jnp.float32).reshape(rows * blocks, BLOCK)
    return tail(keep, res, norm_gain.reshape(blocks, BLOCK), swap(send, mask), rows)


def solution(mesh):
    step = jax.shard_map(
        local,
        mesh=mesh,
        in_specs=(P("dp", "tensor"), P("tensor", None), P(("dp", "tensor"), None), P()),
        out_specs=(P(("dp", "tensor"), None), P(("dp", "tensor"), None), P(("dp", "tensor"), None)),
        check_vma=False,
    )
    return step
```

```python
import functools
import jax
import jax.numpy as jnp
from jax import lax
from jax.experimental import pallas as pl
from jax.experimental.pallas import tpu as pltpu
from jax.sharding import PartitionSpec as P

BLOCK = 128
AXIS = "tensor"
MIB = 1024 * 1024
LEAD = 2
NEAR = 4
STRIP = 4


def up(value, step):
    return -(-value // step) * step


def product_kernel(lots, rows, strips, attn_hbm, w_ref, *refs):
    count = len(lots)
    outs, (attn_ref, w_buf, sems, attn_sem) = refs[:count], refs[count:]
    tokens = attn_ref.shape[0]
    blocks = w_ref.shape[1] // BLOCK
    held = [len(lot) * rows for lot in lots]
    first = [sum(up(h, 8) for h in held[:k]) for k in range(count + 1)]
    fetch = pltpu.make_async_copy(attn_hbm, attn_ref, attn_sem)
    fetch.start()
    spans = [pl.ds(start * BLOCK, wide * BLOCK) for start, wide in strips]
    copies = [pltpu.make_async_copy(w_ref.at[:, span], w_buf.at[:, span], sems.at[s]) for s, span in enumerate(spans)]
    for copy in copies[:LEAD]:
        copy.start()
    me = lax.axis_index(AXIS)
    pos = lax.broadcasted_iota(jnp.int32, (first[-1], tokens), 0)
    col = lax.broadcasted_iota(jnp.int32, (first[-1], tokens), 1)
    want = jnp.full_like(pos, -1)
    for k, lot in enumerate(lots):
        for f, mask in enumerate(lot):
            start = first[k] + f * rows
            here = (pos >= start) & (pos < start + rows)
            want = jnp.where(here, (me ^ mask) * rows + pos - start, want)
    pick = jnp.where(col == want, 1.0, 0.0).astype(jnp.bfloat16)
    fetch.wait()
    for copy in copies[LEAD:]:
        copy.start()
    mine = jnp.dot(pick, attn_ref[...], preferred_element_type=jnp.float32).astype(jnp.bfloat16)
    for s, (start, wide) in enumerate(strips):
        copies[s].wait()
        acc = jnp.dot(mine, w_buf[:, spans[s]], preferred_element_type=jnp.float32)
        for c in range(wide):
            for k, out in enumerate(outs):
                out[pl.ds(start + c, held[k], stride=blocks), :] = acc[
                    first[k] : first[k] + held[k], c * BLOCK : (c + 1) * BLOCK
                ]


def cut(blocks):
    return [(start, min(STRIP, blocks - start)) for start in range(0, blocks, STRIP)]


def product(attn, w, lots, rows):
    tokens, depth = attn.shape
    width = w.shape[1]
    strips = cut(width // BLOCK)
    return pl.pallas_call(
        functools.partial(product_kernel, lots, rows, strips),
        out_shape=[
            jax.ShapeDtypeStruct((len(lot) * rows * width // BLOCK, BLOCK), jnp.float32) for lot in lots
        ],
        in_specs=[pl.BlockSpec(memory_space=pl.ANY)] * 2,
        out_specs=[pl.BlockSpec(memory_space=pltpu.VMEM)] * len(lots),
        scratch_shapes=[
            pltpu.VMEM((tokens, depth), jnp.bfloat16),
            pltpu.VMEM((depth, width), jnp.bfloat16),
            pltpu.SemaphoreType.DMA((len(strips),)),
            pltpu.SemaphoreType.DMA,
        ],
        compiler_params=pltpu.CompilerParams(vmem_limit_bytes=40 * MIB),
        cost_estimate=pl.CostEstimate(
            flops=2 * tokens * depth * width, bytes_accessed=2 * depth * width, transcendentals=0
        ),
        name="product",
    )(pltpu.with_memory_space_constraint(attn, pltpu.HBM), pltpu.with_memory_space_constraint(w, pltpu.HBM))


def fold_kernel(*refs):
    ins, (keep_ref, send_ref) = refs[:-2], refs[-2:]
    half = keep_ref.shape[0]
    for out, start in ((keep_ref, 0), (send_ref, half)):
        lines = pl.ds(start, half)
        value = ins[0][lines, :]
        for ref in ins[1:]:
            value = value + ref[lines, :]
        out[...] = value


def fold(parts):
    half = jax.ShapeDtypeStruct((parts[0].shape[0] // 2, BLOCK), jnp.float32)
    return pl.pallas_call(
        fold_kernel,
        out_shape=[half] * 2,
        in_specs=[pl.BlockSpec(memory_space=pltpu.VMEM)] * len(parts),
        out_specs=[pl.BlockSpec(memory_space=pltpu.VMEM)] * 2,
        compiler_params=pltpu.CompilerParams(vmem_limit_bytes=12 * MIB),
        name="fold",
    )(*parts)


def tail_kernel(rows, gain_ref, *refs):
    terms, (new_ref, quant_ref, scale_ref, hid, nrm) = refs[:-5], refs[-5:]
    blocks = gain_ref.shape[0]
    line = lax.broadcasted_iota(jnp.int32, (blocks, BLOCK), 0)
    lane = lax.broadcasted_iota(jnp.int32, (blocks, BLOCK), 1)
    for j in range(rows):
        at = pl.ds(j * blocks, blocks)
        hidden = terms[0][at, :]
        for term in terms[1:]:
            hidden = hidden + term[at, :]
        hid[at, :] = hidden
        square = jnp.sum(jnp.sum(hidden * hidden, axis=0, keepdims=True), axis=1, keepdims=True)
        normed = hidden * lax.rsqrt(square / (blocks * BLOCK) + 1e-06) * gain_ref[...]
        peak = jnp.max(jnp.abs(normed), axis=1, keepdims=True) + 1e-06
        nrm[at, :] = normed * 448.0 / peak
        spread = jnp.where(line == lane, peak / 448.0, 0.0)
        scale_ref[pl.ds(j, 1), :] = jnp.sum(spread, axis=0, keepdims=True)[:, :blocks]
    for c in range(blocks):
        lanes = pl.ds(c * BLOCK, BLOCK)
        new_ref[:, lanes] = hid[pl.ds(c, rows, stride=blocks), :].astype(jnp.bfloat16)
        quant_ref[:, lanes] = nrm[pl.ds(c, rows, stride=blocks), :].astype(jnp.bfloat16)


def tail(gain, terms, rows):
    blocks = gain.shape[0]
    width = blocks * BLOCK
    return pl.pallas_call(
        functools.partial(tail_kernel, rows),
        out_shape=(
            jax.ShapeDtypeStruct((rows, width), jnp.bfloat16),
            jax.ShapeDtypeStruct((rows, width), jnp.bfloat16),
            jax.ShapeDtypeStruct((rows, blocks), jnp.float32),
        ),
        in_specs=[pl.BlockSpec(memory_space=pltpu.VMEM)] * (1 + len(terms)),
        out_specs=[pl.BlockSpec(memory_space=pltpu.VMEM)] * 3,
        scratch_shapes=[pltpu.VMEM((rows * blocks, BLOCK), jnp.float32)] * 2,
        compiler_params=pltpu.CompilerParams(vmem_limit_bytes=8 * MIB),
        name="tail",
    )(gain, *terms)


def local(attn_out, w_out, residual, norm_gain):
    groups = lax.axis_size(AXIS)
    rows, width = residual.shape
    blocks = width // BLOCK
    if groups < 2 * NEAR or groups & (groups - 1):
        raise ValueError("groups")
    far = groups // NEAR

    def swap(value, mask):
        return lax.ppermute(value, AXIS, [(i, i ^ mask) for i in range(groups)])

    spread = [f * NEAR for f in range(far)]
    low, high = spread[: far // 2], spread[far // 2 :]
    top = groups // 2
    lots = [[q + f for f in spread] for q in range(NEAR - 1)]
    lots += [[NEAR - 1 + f for f in low], [NEAR - 1 + f for f in high]]
    own, one, two, three, cross = product(attn_out, w_out, lots, rows)
    one, two = swap(one, 1), swap(two, 2)
    cross, three = swap(cross, NEAR - 1 + top), swap(three, NEAR - 1)
    keep, send = fold([own, one, two])
    terms = [keep, three, cross, swap(send, top)]
    while top > NEAR:
        top //= 2
        keep, send = fold(terms)
        terms = [keep, swap(send, top)]
    res = residual.astype(jnp.float32).reshape(rows * blocks, BLOCK)
    return tail(norm_gain.reshape(blocks, BLOCK), [res, *terms], rows)


def solution(mesh):
    return jax.shard_map(
        local,
        mesh=mesh,
        in_specs=(P("dp", "tensor"), P("tensor", None), P(("dp", "tensor"), None), P()),
        out_specs=(P(("dp", "tensor"), None), P(("dp", "tensor"), None), P(("dp", "tensor"), None)),
        check_vma=False,
    )
```

```python
import functools
import jax
import jax.numpy as jnp
from jax import lax
from jax.experimental import pallas as pl
from jax.experimental.pallas import tpu as pltpu
from jax.sharding import PartitionSpec as P

BLOCK = 128
AXIS = "tensor"
MIB = 1024 * 1024
LEAD = 2
NEAR = 4
STRIP = 4


def up(value, step):
    return -(-value // step) * step


def product_kernel(lots, rows, strips, attn_hbm, w_ref, *refs):
    count = len(lots)
    outs, (attn_ref, w_buf, sems, attn_sem) = refs[:count], refs[count:]
    tokens = attn_ref.shape[0]
    blocks = w_ref.shape[1] // BLOCK
    held = [len(lot) * rows for lot in lots]
    first = [sum(up(h, 8) for h in held[:k]) for k in range(count + 1)]
    fetch = pltpu.make_async_copy(attn_hbm, attn_ref, attn_sem)
    fetch.start()
    spans = [pl.ds(start * BLOCK, wide * BLOCK) for start, wide in strips]
    copies = [pltpu.make_async_copy(w_ref.at[:, span], w_buf.at[:, span], sems.at[s]) for s, span in enumerate(spans)]
    for copy in copies[:LEAD]:
        copy.start()
    me = lax.axis_index(AXIS)
    pos = lax.broadcasted_iota(jnp.int32, (first[-1], tokens), 0)
    col = lax.broadcasted_iota(jnp.int32, (first[-1], tokens), 1)
    want = jnp.full_like(pos, -1)
    for k, lot in enumerate(lots):
        for f, mask in enumerate(lot):
            start = first[k] + f * rows
            here = (pos >= start) & (pos < start + rows)
            want = jnp.where(here, (me ^ mask) * rows + pos - start, want)
    pick = jnp.where(col == want, 1.0, 0.0).astype(jnp.bfloat16)
    fetch.wait()
    for copy in copies[LEAD:]:
        copy.start()
    mine = jnp.dot(pick, attn_ref[...], preferred_element_type=jnp.float32).astype(jnp.bfloat16)
    for s, (start, wide) in enumerate(strips):
        copies[s].wait()
        acc = jnp.dot(mine, w_buf[:, spans[s]], preferred_element_type=jnp.float32)
        for c in range(wide):
            for k, out in enumerate(outs):
                out[pl.ds(start + c, held[k], stride=blocks), :] = acc[
                    first[k] : first[k] + held[k], c * BLOCK : (c + 1) * BLOCK
                ]


def cut(blocks):
    return [(start, min(STRIP, blocks - start)) for start in range(0, blocks, STRIP)]


def product(attn, w, lots, rows):
    tokens, depth = attn.shape
    width = w.shape[1]
    strips = cut(width // BLOCK)
    return pl.pallas_call(
        functools.partial(product_kernel, lots, rows, strips),
        out_shape=[
            jax.ShapeDtypeStruct((len(lot) * rows * width // BLOCK, BLOCK), jnp.float32) for lot in lots
        ],
        in_specs=[pl.BlockSpec(memory_space=pl.ANY)] * 2,
        out_specs=[pl.BlockSpec(memory_space=pltpu.VMEM)] * len(lots),
        scratch_shapes=[
            pltpu.VMEM((tokens, depth), jnp.bfloat16),
            pltpu.VMEM((depth, width), jnp.bfloat16),
            pltpu.SemaphoreType.DMA((len(strips),)),
            pltpu.SemaphoreType.DMA,
        ],
        compiler_params=pltpu.CompilerParams(vmem_limit_bytes=40 * MIB),
        cost_estimate=pl.CostEstimate(
            flops=2 * tokens * depth * width, bytes_accessed=2 * depth * width, transcendentals=0
        ),
        name="product",
    )(pltpu.with_memory_space_constraint(attn, pltpu.HBM), pltpu.with_memory_space_constraint(w, pltpu.HBM))


def fold_kernel(*refs):
    ins, send_ref = refs[:-1], refs[-1]
    half = send_ref.shape[0]
    value = ins[0][pl.ds(half, half), :]
    for ref in ins[1:]:
        value = value + ref[pl.ds(half, half), :]
    send_ref[...] = value


def fold(parts):
    return pl.pallas_call(
        fold_kernel,
        out_shape=jax.ShapeDtypeStruct((parts[0].shape[0] // 2, BLOCK), jnp.float32),
        in_specs=[pl.BlockSpec(memory_space=pltpu.VMEM)] * len(parts),
        out_specs=pl.BlockSpec(memory_space=pltpu.VMEM),
        compiler_params=pltpu.CompilerParams(vmem_limit_bytes=12 * MIB),
        name="fold",
    )(*parts)


def tail_kernel(rows, gain_ref, *refs):
    terms, (new_ref, quant_ref, scale_ref, hid, nrm) = refs[:-5], refs[-5:]
    blocks = gain_ref.shape[0]
    line = lax.broadcasted_iota(jnp.int32, (blocks, BLOCK), 0)
    lane = lax.broadcasted_iota(jnp.int32, (blocks, BLOCK), 1)
    for j in range(rows):
        at = pl.ds(j * blocks, blocks)
        hidden = terms[0][at, :]
        for term in terms[1:]:
            hidden = hidden + term[at, :]
        hid[at, :] = hidden
        square = jnp.sum(jnp.sum(hidden * hidden, axis=0, keepdims=True), axis=1, keepdims=True)
        normed = hidden * lax.rsqrt(square / (blocks * BLOCK) + 1e-06) * gain_ref[...]
        peak = jnp.max(jnp.abs(normed), axis=1, keepdims=True) + 1e-06
        nrm[at, :] = normed * 448.0 / peak
        spread = jnp.where(line == lane, peak / 448.0, 0.0)
        scale_ref[pl.ds(j, 1), :] = jnp.sum(spread, axis=0, keepdims=True)[:, :blocks]
    for c in range(blocks):
        lanes = pl.ds(c * BLOCK, BLOCK)
        new_ref[:, lanes] = hid[pl.ds(c, rows, stride=blocks), :].astype(jnp.bfloat16)
        quant_ref[:, lanes] = nrm[pl.ds(c, rows, stride=blocks), :].astype(jnp.bfloat16)


def tail(gain, terms, rows):
    blocks = gain.shape[0]
    width = blocks * BLOCK
    return pl.pallas_call(
        functools.partial(tail_kernel, rows),
        out_shape=(
            jax.ShapeDtypeStruct((rows, width), jnp.bfloat16),
            jax.ShapeDtypeStruct((rows, width), jnp.bfloat16),
            jax.ShapeDtypeStruct((rows, blocks), jnp.float32),
        ),
        in_specs=[pl.BlockSpec(memory_space=pltpu.VMEM)] * (1 + len(terms)),
        out_specs=[pl.BlockSpec(memory_space=pltpu.VMEM)] * 3,
        scratch_shapes=[pltpu.VMEM((rows * blocks, BLOCK), jnp.float32)] * 2,
        compiler_params=pltpu.CompilerParams(vmem_limit_bytes=8 * MIB),
        name="tail",
    )(gain, *terms)


def local(attn_out, w_out, residual, norm_gain):
    groups = lax.axis_size(AXIS)
    rows, width = residual.shape
    blocks = width // BLOCK
    if groups < 2 * NEAR or groups & (groups - 1):
        raise ValueError("groups")
    far = groups // NEAR

    def swap(value, mask):
        return lax.ppermute(value, AXIS, [(i, i ^ mask) for i in range(groups)])

    spread = [f * NEAR for f in range(far)]
    low, high = spread[: far // 2], spread[far // 2 :]
    top = groups // 2
    lots = [[q + f for f in spread] for q in range(NEAR - 1)]
    lots += [[NEAR - 1 + f for f in low], [NEAR - 1 + f for f in high]]
    own, one, two, three, cross = product(attn_out, w_out, lots, rows)
    one, two = swap(one, 1), swap(two, 2)
    cross, three = swap(cross, NEAR - 1 + top), swap(three, NEAR - 1)
    send = fold([own, one, two])
    terms = [own, one, two, three, cross, swap(send, top)]
    while top > NEAR:
        top //= 2
        sums = functools.reduce(jnp.add, [term[: terms[-1].shape[0]] for term in terms])
        half = sums.shape[0] // 2
        terms = [sums[:half], swap(sums[half:], top)]
    res = residual.astype(jnp.float32).reshape(rows * blocks, BLOCK)
    return tail(norm_gain.reshape(blocks, BLOCK), [res, *terms], rows)


def solution(mesh):
    return jax.shard_map(
        local,
        mesh=mesh,
        in_specs=(P("dp", "tensor"), P("tensor", None), P(("dp", "tensor"), None), P()),
        out_specs=(P(("dp", "tensor"), None), P(("dp", "tensor"), None), P(("dp", "tensor"), None)),
        check_vma=False,
    )
```
